32 devices in a mesh: member: 8 (over y, x, core), domain: 4 (over z).
Axes of the slice: x: 2, y: 2, z: 4, core: 2. Of those that a mesh axis runs over, the one named last changes fastest.
Arguments:
- ensemble: bfloat16 [256, 2, 16, 512], P('member', None, None, 'domain'), may hold values from -4 to 4
- obs_value: float32 [8, 1024], P('member', 'domain'), may hold values from -6 to 6
- obs_prec: float32 [8, 1024], P('member', 'domain'), may hold values from 1 to 10
- obs_row: int32 [8, 1024], P('member', 'domain'), may hold values from 0 to 1
- obs_col: int32 [8, 1024], P('member', 'domain'), may hold values from 0 to 127
- loc_mask: int32 [8, 16], P('member', 'domain'), may hold values 0 or 1
Outputs:
- analysis: bfloat16 [256, 2, 16, 512], P('member', None, None, 'domain')
The draws below stay inside these ranges and needn't reach their ends.
All inputs are finite; a program needn't handle non-finite values. No bound on the sum of `loc_mask` on one device may be relied on, other than what follows from the above.
Results may differ from the reference program's by a relative error of at most 0.0075.
Values may be sent and summed in bfloat16 or wider, within the bound.
A program may use at most 64 MiB of HBM per device.

```python
import math
import jax
import jax.numpy as jnp
from jax import lax

MEMBERS = 256
REGION_ROWS = 2
REGION_COLUMNS = 128
P_OWN = 256
ROWS = 16
COLS = 512
OBS_COLS = 1024
MASK_COLS = 16
N_MEMBER = 8
N_DOMAIN = 4


def plant(entries, stream_key, smallest, top_value):
    longest = entries.shape.index(max(entries.shape))
    spots = []
    for shift in (0, 1):
        where = [jax.random.randint(jax.random.fold_in(stream_key, axis), (), 0, length) for axis, length in enumerate(entries.shape)]
        where[longest] = (where[longest] + shift) % entries.shape[longest]
        spots.append(tuple(where))
    return entries.at[spots[0]].set(smallest).at[spots[1]].set(top_value)


def level_of(stream_key, dims, shards, smallest, high):
    factor_of = 1.0
    for dim, blocks in shards:
        draws = jax.random.uniform(jax.random.fold_in(jax.random.fold_in(stream_key, 6), dim), (blocks,), jnp.float32, smallest / len(shards), high / len(shards))
        factor_of = factor_of * jnp.repeat(jnp.exp(draws), dims[dim] // blocks).reshape((-1,) + (1,) * (len(dims) - 1 - dim))
    return factor_of


def bell_draw(own_key, dims, spread, most, pieces=(), kind=jnp.bfloat16):
    loudness = level_of(own_key, dims, pieces, -0.22, 0.18) if pieces else 1.0
    entries = jax.random.normal(own_key, dims, jnp.float32) * spread * loudness
    return jnp.minimum(jnp.maximum(entries, -most), most).astype(kind)


def setup_inputs(seed: int = 0) -> dict:
    key_list = jax.random.split(jax.random.key(seed), 7)
    ensemble = bell_draw(key_list[0], (MEMBERS, 2, ROWS, COLS), 1.0, 4.0, ((0, 8), (3, 4)))
    obs_value = bell_draw(key_list[1], (N_MEMBER, OBS_COLS), 1.0, 6.0, ((0, 8), (1, 4)), jnp.float32)
    obs_prec = jnp.clip(jnp.exp(math.log(10.0) - 2.3025851 * jax.random.uniform(key_list[2], (N_MEMBER, OBS_COLS), jnp.float32) ** level_of(key_list[2], (N_MEMBER, OBS_COLS), ((0, 8), (1, 4)), -0.2, 0.2)), 1.0, 10.0)
    obs_row = plant(jax.random.randint(key_list[3], (N_MEMBER, OBS_COLS), 0, REGION_ROWS), jax.random.fold_in(key_list[3], 1), 0, REGION_ROWS - 1).astype(jnp.int32)
    obs_col = plant(jax.random.randint(key_list[4], (N_MEMBER, OBS_COLS), 0, REGION_COLUMNS), jax.random.fold_in(key_list[4], 1), 0, REGION_COLUMNS - 1).astype(jnp.int32)
    loc_mask = plant((jax.random.randint(key_list[5], (N_MEMBER, MASK_COLS), 0, 4) < 3).astype(jnp.int32), jax.random.fold_in(key_list[5], 1), 0, 1)
    return {"ensemble": ensemble, "obs_value": obs_value, "obs_prec": obs_prec, "obs_row": obs_row, "obs_col": obs_col, "loc_mask": loc_mask}


ADVECT = 0.4
DIFFUSE = 0.15
OBS_WIND = 0.5

def step_forward(central_cell, east_cells, west_cells, north_cells, south_cells):
    middle = central_cell.astype(jnp.float32)
    east_side = east_cells.astype(jnp.float32)
    west_side = west_cells.astype(jnp.float32)
    laplace = east_side + west_side + north_cells.astype(jnp.float32) + south_cells.astype(jnp.float32) - 4.0 * middle
    wind_field = middle[:, 0:1]
    return (middle - ADVECT * 0.5 * wind_field * (east_side - west_side) + DIFFUSE * laplace).astype(jnp.bfloat16)

def observe(local_region, obs_index, observed, precision):
    member_states = local_region.shape[0]
    wind_field = local_region[:, 0].reshape(member_states, -1)
    tracer = local_region[:, 1].reshape(member_states, -1)
    equivalent = jnp.take(tracer, obs_index, axis=1).astype(jnp.float32) + OBS_WIND * jnp.take(wind_field, obs_index, axis=1).astype(jnp.float32)
    central_cell = lax.optimization_barrier(jnp.mean(equivalent, axis=0))
    scaled = (equivalent - central_cell) * (member_states - 1) ** (-0.5)
    return jnp.concatenate([scaled, (observed - central_cell)[None], precision[None]], axis=0).astype(jnp.bfloat16)

def block_weights(local_rows, block_mask, parts):
    member_states = local_rows.shape[0] - 2
    tapering = jnp.array([0.5, 1.0, 1.0, 0.5], jnp.float32) * block_mask.astype(jnp.float32)
    block_cols = local_rows.shape[1] // len(parts)
    factor = jnp.repeat(tapering[jnp.array(parts)], block_cols)
    return local_rows[member_states + 1].astype(jnp.float32) * factor

def contributions(local_rows, weight):
    member_states = local_rows.shape[0] - 2
    anomaly_obs = local_rows[:member_states]
    innovation = local_rows[member_states].astype(jnp.float32)
    weighted = (anomaly_obs.astype(jnp.float32) * weight).astype(jnp.bfloat16)
    cross_term = lax.dot_general(weighted, anomaly_obs, (((1,), (1,)), ((), ())), preferred_element_type=jnp.float32)
    forcing = jnp.dot(weighted.astype(jnp.float32), innovation, precision=lax.Precision.HIGHEST)
    return (cross_term, forcing)

def analyse(local_region, cross_term, forcing):
    member_states = local_region.shape[0]
    cells = local_region.reshape(member_states, -1)
    ens_mean = lax.optimization_barrier(jnp.mean(cells.astype(jnp.float32), axis=0))
    anomalies = (cells.astype(jnp.float32) - ens_mean).astype(jnp.bfloat16)
    identity = jnp.eye(member_states, dtype=jnp.float32)
    cross_half = cross_term.astype(jnp.bfloat16)
    squared = jnp.dot(cross_half, cross_half, preferred_element_type=jnp.float32)
    row_bound = jnp.sqrt(jnp.max(lax.optimization_barrier(jnp.sum(jnp.abs(squared), axis=1))))
    half_width = (row_bound + 1.0) / 2.0
    theta = 1.0 + half_width
    ratio_sigma = theta / half_width
    rho_first = 1.0 / ratio_sigma
    first_resid = (1.0 - 1.0 / theta) * identity - cross_term / theta
    first_step = first_resid / theta
    applied = first_step + ((theta - 1.0) * cross_term - squared) / (theta * theta)
    second_resid = first_resid - applied
    rho_second = 1.0 / (2.0 * ratio_sigma - rho_first)
    second_step = rho_second * rho_first * first_step + 2.0 * rho_second / half_width * second_resid
    inverse = identity / theta + first_step + second_step
    mean_weights = jnp.dot(inverse, forcing, precision=lax.Precision.HIGHEST)
    transform = (0.5 * (identity + inverse) + mean_weights[:, None] * (member_states - 1) ** (-0.5)).astype(jnp.bfloat16)
    increment = lax.dot_general(transform, anomalies, (((0,), (0,)), ((), ())), preferred_element_type=jnp.float32)
    return (ens_mean + increment).astype(jnp.bfloat16).reshape(local_region.shape)

def reference(ensemble, obs_value, obs_prec, obs_row, obs_col, loc_mask):
    member_states = ensemble.shape[0]
    padded_region = jnp.concatenate([ensemble[..., -1:], ensemble, ensemble[..., :1]], axis=3)
    central_cell = padded_region[..., 1:-1]
    predicted_state = step_forward(central_cell, padded_region[..., 2:], padded_region[..., :-2], jnp.roll(central_cell, -1, axis=2), jnp.roll(central_cell, 1, axis=2))
    fixed_point = jnp.zeros((), jnp.int32)
    count = N_MEMBER * N_DOMAIN
    half_cols = P_OWN // 2

    def region_of(region_id):
        row_strip = (region_id // N_DOMAIN).astype(jnp.int32)
        column_block = (region_id % N_DOMAIN).astype(jnp.int32)
        local_region = lax.dynamic_slice(predicted_state, (fixed_point, fixed_point, row_strip * REGION_ROWS, column_block * REGION_COLUMNS), (member_states, 2, REGION_ROWS, REGION_COLUMNS))
        return (local_region, row_strip, column_block)

    def make_rows(region_id):
        local_region, row_strip, column_block = region_of(region_id)
        start = column_block * P_OWN
        observed = lax.dynamic_slice(obs_value, (row_strip, start), (1, P_OWN))[0]
        precision = lax.dynamic_slice(obs_prec, (row_strip, start), (1, P_OWN))[0]
        rows_at = lax.dynamic_slice(obs_row, (row_strip, start), (1, P_OWN))[0]
        cols_at = lax.dynamic_slice(obs_col, (row_strip, start), (1, P_OWN))[0]
        return observe(local_region, rows_at * REGION_COLUMNS + cols_at, observed, precision)
    stacked = lax.map(make_rows, jnp.arange(count, dtype=jnp.int32))

    def make_analysis(region_id):
        local_region, row_strip, column_block = region_of(region_id)
        left_id = row_strip * N_DOMAIN + (column_block + N_DOMAIN - 1) % N_DOMAIN
        right_id = row_strip * N_DOMAIN + (column_block + 1) % N_DOMAIN
        local_rows = jnp.concatenate([stacked[left_id][:, half_cols:], stacked[region_id], stacked[right_id][:, :half_cols]], axis=1)
        block_mask = lax.dynamic_slice(loc_mask, (row_strip, column_block * 4), (1, 4))[0]
        weight = block_weights(local_rows, block_mask, [0, 1, 2, 3])
        cross_term, forcing = contributions(local_rows, weight)
        return analyse(local_region, cross_term, forcing)
    results = lax.map(make_analysis, jnp.arange(count, dtype=jnp.int32))
    results = results.reshape(N_MEMBER, N_DOMAIN, member_states, 2, REGION_ROWS, REGION_COLUMNS)
    results = jnp.transpose(results, (2, 3, 0, 4, 1, 5))
    return results.reshape(member_states, 2, REGION_ROWS * N_MEMBER, REGION_COLUMNS * N_DOMAIN)
```

```python
import functools

import jax
import jax.numpy as jnp
from jax import lax
from jax.experimental import pallas as pl
from jax.experimental.pallas import tpu as pltpu
from jax.sharding import PartitionSpec as P

ADVECT = 0.4
DIFFUSE = 0.15
OBS_WIND = 0.5
TAPER = (0.5, 1.0, 1.0, 0.5)
MESH = pl.DeviceIdType.MESH
F32 = jnp.float32
BF16 = jnp.bfloat16


def remote(src, dst, send, recv, where):
    return pltpu.make_async_remote_copy(
        src_ref=src, dst_ref=dst, send_sem=send, recv_sem=recv, device_id=where, device_id_type=MESH
    )


def kernel(
    nm, nd, ens, value, prec, row, col, mask, out,
    raw, val_v, prec_v, row_v, col_v, mask_v, rows_f32, halo_out, halo_in, bands, cells, obs_own, obs_in,
    back, got, load_sem, halo_send, halo_recv, out_send, out_recv, obs_send, obs_recv, back_send, back_recv,
):
    me_m = lax.axis_index("member")
    me_d = lax.axis_index("domain")
    east = lax.rem(me_d + 1, nd)
    west = lax.rem(me_d + nd - 1, nd)
    peers = [lax.rem(me_m + i, nm) for i in range(nm)]
    froms = [lax.rem(me_m + nm - i, nm) for i in range(nm)]
    own, fields, nrows, ncols = raw.shape
    reg = nrows // nm
    members = own * nm
    pitch = fields * nrows

    barrier = pltpu.get_barrier_semaphore()
    for i in range(1, nm):
        pl.semaphore_signal(barrier, inc=1, device_id={"member": peers[i]}, device_id_type=MESH)
    for near in (east, west):
        pl.semaphore_signal(barrier, inc=1, device_id={"domain": near}, device_id_type=MESH)
    loads = [
        pltpu.make_async_copy(src, dst, load_sem.at[i])
        for i, (src, dst) in enumerate(
            [(ens, raw), (value, val_v), (prec, prec_v), (row, row_v), (col, col_v), (mask, mask_v)]
        )
    ]
    for load in loads:
        load.start()
    loads[0].wait()

    rows_f32[...] = raw[...].astype(F32).reshape(own * pitch, ncols)

    def line(f, r):
        return rows_f32[pl.ds(f * nrows + r % nrows, own, stride=pitch), :]

    lane = lax.broadcasted_iota(jnp.int32, (own, ncols), 1)
    first = jnp.zeros((own, ncols), F32)
    last = jnp.zeros((own, ncols), F32)
    for f in range(fields):
        for r in range(nrows):
            spot = f * nrows + r
            here = line(f, r)
            first = jnp.where(lane == spot, pltpu.roll(here, spot % ncols, 1), first)
            last = jnp.where(lane == spot, pltpu.roll(here, (spot + 1) % ncols, 1), last)
    halo_out[0] = first.astype(BF16)
    halo_out[1] = last.astype(BF16)
    pl.semaphore_wait(barrier, nm + 1)
    halos = [
        remote(halo_out.at[0], halo_in.at[0], halo_send.at[0], halo_recv.at[0], {"domain": west}),
        remote(halo_out.at[1], halo_in.at[1], halo_send.at[1], halo_recv.at[1], {"domain": east}),
    ]
    for copy in halos:
        copy.start()
    for load in loads[1:]:
        load.wait()
    nobs = val_v.shape[1]
    half = nobs // 2
    index = row_v[...] * ncols + col_v[...]
    spots = lax.broadcasted_iota(jnp.int32, (reg * ncols, nobs), 0)
    hit = jnp.where(spots == index, 1.0, 0.0)
    pick = jnp.concatenate([(OBS_WIND * hit).astype(BF16), hit.astype(BF16)], axis=0)
    for copy in halos:
        copy.wait_recv()

    from_east = halo_in[0].astype(F32)
    from_west = halo_in[1].astype(F32)

    def forecast(f, r):
        spot = f * nrows + r
        middle = line(f, r)
        shape = middle.shape
        east_side = jnp.where(
            lane == ncols - 1,
            jnp.broadcast_to(from_east[:, spot : spot + 1], shape),
            pltpu.roll(middle, ncols - 1, 1),
        )
        west_side = jnp.where(
            lane == 0, jnp.broadcast_to(from_west[:, spot : spot + 1], shape), pltpu.roll(middle, 1, 1)
        )
        laplace = east_side + west_side + line(f, r + 1) + line(f, r - 1) - 4.0 * middle
        return (
            middle - ADVECT * 0.5 * line(0, r) * (east_side - west_side) + DIFFUSE * laplace
        ).astype(BF16)

    for m in range(nm):
        for f in range(fields):
            for r in range(reg):
                bands[m, f * reg + r] = forecast(f, m * reg + r)

    def mine(block):
        return pl.ds(pl.multiple_of(block * own, own), own)

    sends = []
    for i in range(1, nm):
        copy = remote(
            bands.at[peers[i]], cells.at[:, mine(me_m), :], out_send.at[i], out_recv.at[i], {"member": peers[i]}
        )
        copy.start()
        sends.append(copy)
    cells[:, mine(me_m), :] = bands[me_m]
    for i in range(1, nm):
        remote(
            bands.at[froms[i]], cells.at[:, mine(froms[i]), :], out_send.at[i], out_recv.at[i], {"member": froms[i]}
        ).wait_recv()

    count = fields * reg
    state = jnp.concatenate([cells[i] for i in range(count)], axis=1)
    equivalent = jnp.dot(state, pick, preferred_element_type=F32)
    center = jnp.sum(equivalent, axis=0, keepdims=True) * (1.0 / members)
    scaled = ((equivalent - center) * (members - 1) ** (-0.5)).astype(BF16)
    tail_row = lax.broadcasted_iota(jnp.int32, (16, nobs), 0)
    tail = jnp.where(
        tail_row == 0, val_v[...] - center, jnp.where(tail_row == 1, prec_v[...], 0.0)
    ).astype(BF16)
    for side in range(2):
        part = slice(side * half, (side + 1) * half)
        obs_own[side, 0:members] = scaled[:, part]
        obs_own[side, members : members + 16] = tail[:, part]
    swaps = [
        remote(obs_own.at[0], obs_in.at[1], obs_send.at[0], obs_recv.at[1], {"domain": west}),
        remote(obs_own.at[1], obs_in.at[0], obs_send.at[1], obs_recv.at[0], {"domain": east}),
    ]
    for copy in swaps:
        copy.start()

    wide = state.astype(F32)
    ens_mean = jnp.sum(wide, axis=0, keepdims=True) * (1.0 / members)
    anomalies = (wide - ens_mean).astype(BF16)

    def term(block, which):
        rows = block[0:members]
        ends = block[members : members + 16]
        use = TAPER[which] * mask_v[0:1, which : which + 1].astype(F32)
        weight = ends[1:2].astype(F32) * use
        weighted = (rows.astype(F32) * weight).astype(BF16)
        part = lax.dot_general(rows, weighted, (((1,), (1,)), ((), ())), preferred_element_type=F32)
        push = lax.dot_general(weighted, ends, (((1,), (1,)), ((), ())), preferred_element_type=F32)
        return part, push[:, 0:1]

    cross, forcing = term(obs_own[0], 1)
    more, push = term(obs_own[1], 2)
    cross, forcing = cross + more, forcing + push
    swaps[1].wait_recv()
    more, push = term(obs_in[0], 0)
    cross, forcing = cross + more, forcing + push
    swaps[0].wait_recv()
    more, push = term(obs_in[1], 3)
    cross, forcing = cross + more, forcing + push

    cross_half = cross.astype(BF16)
    squared = jnp.dot(cross_half, cross_half, preferred_element_type=F32)
    sums = jnp.sum(jnp.abs(squared), axis=0, keepdims=True)
    bound = jnp.sqrt(jnp.max(sums, axis=1, keepdims=True))
    delta = (bound + 1.0) / 2.0
    theta = 1.0 + delta
    sigma = theta / delta
    rho0 = 1.0 / sigma
    rho1 = 1.0 / (2.0 * sigma - rho0)
    rest = 1.0 - 1.0 / theta
    keep = 1.0 + rho1 * rho0
    on_eye = 1.0 / theta + keep * rest / theta + 2.0 * rho1 / delta * rest * rest
    on_cross = -(keep + 4.0 * rho1) / (theta * theta)
    on_square = 2.0 * rho1 / (delta * theta * theta)
    eye = lax.broadcasted_iota(jnp.int32, (members, members), 0) == lax.broadcasted_iota(
        jnp.int32, (members, members), 1
    )
    inverse = jnp.where(eye, on_eye, 0.0) + on_cross * cross + on_square * squared
    mean_weights = jnp.sum(inverse * forcing, axis=0, keepdims=True)
    transform = (
        0.5 * (jnp.where(eye, 1.0, 0.0) + inverse) + mean_weights * (members - 1) ** (-0.5)
    ).astype(BF16)
    analysis = (
        ens_mean + jnp.dot(transform, anomalies, preferred_element_type=F32)
    ).astype(BF16)
    for i in range(count):
        back[i] = analysis[:, i * ncols : (i + 1) * ncols]
    returns = []
    for i in range(1, nm):
        copy = remote(
            back.at[:, mine(peers[i]), :], got.at[me_m], back_send.at[i], back_recv.at[i], {"member": peers[i]}
        )
        copy.start()
        returns.append(copy)
    got[me_m] = back[:, mine(me_m), :]
    for i in range(1, nm):
        remote(
            back.at[:, mine(froms[i]), :], got.at[froms[i]], back_send.at[i], back_recv.at[i], {"member": froms[i]}
        ).wait_recv()
    for m in range(nm):
        for f in range(fields):
            for r in range(reg):
                rows_f32[pl.ds(f * nrows + m * reg + r, own, stride=pitch), :] = got[m, f * reg + r].astype(F32)
    out[...] = rows_f32[...].reshape(own, fields, nrows, ncols).astype(BF16)
    for copy in halos + sends + swaps + returns:
        copy.wait_send()


def solution(mesh):
    nm, nd = mesh.shape["member"], mesh.shape["domain"]

    def on_device(ensemble, obs_value, obs_prec, obs_row, obs_col, loc_mask):
        own, fields, nrows, ncols = ensemble.shape
        reg = nrows // nm
        members = own * nm
        nobs = obs_value.shape[1]
        vm = pltpu.VMEM
        dma = pltpu.SemaphoreType.DMA
        return pl.pallas_call(
            functools.partial(kernel, nm, nd),
            out_shape=jax.ShapeDtypeStruct(ensemble.shape, BF16),
            in_specs=[pl.BlockSpec(memory_space=pl.ANY)] * 6,
            out_specs=pl.BlockSpec(memory_space=pltpu.VMEM),
            scratch_shapes=[
                vm(ensemble.shape, BF16),
                vm((1, nobs), F32),
                vm((1, nobs), F32),
                vm((1, nobs), jnp.int32),
                vm((1, nobs), jnp.int32),
                vm(loc_mask.shape, jnp.int32),
                vm((own * fields * nrows, ncols), F32),
                vm((2, own, ncols), BF16),
                vm((2, own, ncols), BF16),
                vm((nm, fields * reg, own, ncols), BF16),
                vm((fields * reg, members, ncols), BF16),
                vm((2, members + 16, nobs // 2), BF16),
                vm((2, members + 16, nobs // 2), BF16),
                vm((fields * reg, members, ncols), BF16),
                vm((nm, fields * reg, own, ncols), BF16),
                dma((6,)),
                dma((2,)),
                dma((2,)),
                dma((nm,)),
                dma((nm,)),
                dma((2,)),
                dma((2,)),
                dma((nm,)),
                dma((nm,)),
            ],
            compiler_params=pltpu.CompilerParams(collective_id=0, has_side_effects=True),
        )(ensemble, obs_value, obs_prec, obs_row, obs_col, loc_mask)

    in_specs = (P("member", None, None, "domain"),) + (P("member", "domain"),) * 5
    return jax.shard_map(
        on_device, mesh=mesh, in_specs=in_specs, out_specs=P("member", None, None, "domain"), check_vma=False
    )
```

```python
import functools

import jax
import jax.numpy as jnp
from jax import lax
from jax.experimental import pallas as pl
from jax.experimental.pallas import tpu as pltpu
from jax.sharding import PartitionSpec as P

ADVECT = 0.4
DIFFUSE = 0.15
OBS_WIND = 0.5
TAPER = (0.5, 1.0, 1.0, 0.5)
MESH = pl.DeviceIdType.MESH
F32 = jnp.float32
BF16 = jnp.bfloat16


def remote(src, dst, send, recv, where):
    return pltpu.make_async_remote_copy(
        src_ref=src, dst_ref=dst, send_sem=send, recv_sem=recv, device_id=where, device_id_type=MESH
    )


def kernel(
    nm, nd, ens, value, prec, row, col, mask, got,
    raw, val_v, prec_v, row_v, col_v, mask_v, rows_f32, halo_out, halo_in, bands, cells, edge_out, edge_in, obs_own, obs_in,
    back, load_sem, halo_send, halo_recv, out_send, out_recv, edge_send, edge_recv, obs_send, obs_recv, back_send, back_recv,
):
    me_m = lax.axis_index("member")
    me_d = lax.axis_index("domain")
    east = lax.rem(me_d + 1, nd)
    west = lax.rem(me_d + nd - 1, nd)
    peers = [lax.rem(me_m + i, nm) for i in range(nm)]
    froms = [lax.rem(me_m + nm - i, nm) for i in range(nm)]
    own, fields, nrows, ncols = raw.shape
    reg = nrows // nm
    members = own * nm
    pitch = fields * nrows

    barrier = pltpu.get_barrier_semaphore()
    for i in range(1, nm):
        pl.semaphore_signal(barrier, inc=1, device_id={"member": peers[i]}, device_id_type=MESH)
    for near in (east, west):
        pl.semaphore_signal(barrier, inc=1, device_id={"domain": near}, device_id_type=MESH)
    loads = [
        pltpu.make_async_copy(src, dst, load_sem.at[i])
        for i, (src, dst) in enumerate(
            [(ens, raw), (value, val_v), (prec, prec_v), (row, row_v), (col, col_v), (mask, mask_v)]
        )
    ]
    for load in loads:
        load.start()
    loads[0].wait()

    rows_f32[...] = raw[...].astype(F32).reshape(own * pitch, ncols)

    def line(f, r):
        return rows_f32[pl.ds(f * nrows + (r % nrows if isinstance(r, int) else lax.rem(r, nrows)), own, stride=pitch), :]

    lane = lax.broadcasted_iota(jnp.int32, (own, ncols), 1)
    used = fields * nrows

    def packed(column):
        total = jnp.zeros((own, ncols), F32)
        for f in range(fields):
            for r in range(nrows):
                spot = f * nrows + r
                moved = pltpu.roll(line(f, r), (spot - column) % ncols, 1)
                total = jnp.where(lane == spot, moved, total)
        return total

    first, last = packed(0), packed(ncols - 1)
    halo_out[0] = first.astype(BF16)
    halo_out[1] = last.astype(BF16)
    pl.semaphore_wait(barrier, nm + 1)
    halos = [
        remote(halo_out.at[0], halo_in.at[0], halo_send.at[0], halo_recv.at[0], {"domain": west}),
        remote(halo_out.at[1], halo_in.at[1], halo_send.at[1], halo_recv.at[1], {"domain": east}),
    ]
    for copy in halos:
        copy.start()

    def mine(block):
        return pl.ds(pl.multiple_of(block * own, own), own)

    def step(middle, east_side, west_side, north, south, wind):
        laplace = east_side + west_side + north + south - 4.0 * middle
        return (middle - ADVECT * 0.5 * wind * (east_side - west_side) + DIFFUSE * laplace).astype(BF16)

    def interior(m, f, r):
        at = m * reg + r
        middle = line(f, at)
        return step(
            middle, pltpu.roll(middle, ncols - 1, 1), pltpu.roll(middle, 1, 1),
            line(f, at + 1), line(f, at + nrows - 1), line(0, at),
        )

    sends = []
    for i in list(range(1, nm)) + [0]:
        m = peers[i]
        for f in range(fields):
            for r in range(reg):
                if i:
                    bands[i, f * reg + r] = interior(m, f, r)
                else:
                    cells[f * reg + r, mine(me_m), :] = interior(m, f, r)
        if i:
            copy = remote(bands.at[i], cells.at[:, mine(me_m), :], out_send.at[i], out_recv.at[i], {"member": m})
            copy.start()
            sends.append(copy)

    second, prior = packed(1), packed(ncols - 2)
    row_of = lax.rem(lane, nrows)

    def north_of(x):
        return jnp.where(row_of == nrows - 1, pltpu.roll(x, nrows - 1, 1), pltpu.roll(x, ncols - 1, 1))

    def south_of(x):
        return jnp.where(row_of == 0, pltpu.roll(x, ncols - nrows + 1, 1), pltpu.roll(x, 1, 1))

    def wind_of(x):
        total = x
        for f in range(1, fields):
            total = jnp.where(lane // nrows == f, pltpu.roll(x, f * nrows, 1), total)
        return total

    for copy in halos:
        copy.wait_recv()
    edge_first = step(
        first, second, halo_in[1].astype(F32), north_of(first), south_of(first), wind_of(first)
    )
    edge_last = step(
        last, halo_in[0].astype(F32), prior, north_of(last), south_of(last), wind_of(last)
    )
    layers = edge_out.shape[0]
    if layers == 1:
        edge_out[0] = jnp.where(
            lane < used, edge_first.astype(F32), pltpu.roll(edge_last.astype(F32), used, 1)
        ).astype(BF16)
    else:
        edge_out[0] = edge_first
        edge_out[1] = edge_last
    for i in range(1, nm):
        copy = remote(
            edge_out, edge_in.at[:, mine(me_m), :], edge_send.at[i], edge_recv.at[i], {"member": peers[i]}
        )
        copy.start()
        sends.append(copy)
    for k in range(layers):
        edge_in[k, mine(me_m), :] = edge_out[k]

    for load in loads[1:]:
        load.wait()
    nobs = val_v.shape[1]
    half = nobs // 2
    index = row_v[...] * ncols + col_v[...]
    spots = lax.broadcasted_iota(jnp.int32, (reg * ncols, nobs), 0)
    hit = jnp.where(spots == index, 1.0, 0.0)
    pick = jnp.concatenate([(OBS_WIND * hit).astype(BF16), hit.astype(BF16)], axis=0)

    for i in range(1, nm):
        remote(
            bands.at[i], cells.at[:, mine(froms[i]), :], out_send.at[i], out_recv.at[i], {"member": froms[i]}
        ).wait_recv()
    for i in range(1, nm):
        remote(
            edge_out, edge_in.at[:, mine(froms[i]), :], edge_send.at[i], edge_recv.at[i], {"member": froms[i]}
        ).wait_recv()
    lead = lax.rem(ncols - me_m * reg, ncols)
    edges = [pltpu.roll(edge_in[k].astype(F32), lead, 1) for k in range(layers)]
    wide_lane = lax.broadcasted_iota(jnp.int32, (members, ncols), 1)

    def whole(f, r):
        spot = f * nrows + r
        left = edges[0][:, spot : spot + 1]
        if layers == 1:
            right = edges[0][:, used + spot : used + spot + 1]
        else:
            right = edges[1][:, spot : spot + 1]
        shape = (members, ncols)
        inner = cells[f * reg + r].astype(F32)
        inner = jnp.where(wide_lane == 0, jnp.broadcast_to(left, shape), inner)
        return jnp.where(wide_lane == ncols - 1, jnp.broadcast_to(right, shape), inner)

    count = fields * reg
    wide = jnp.concatenate([whole(f, r) for f in range(fields) for r in range(reg)], axis=1)
    state = wide.astype(BF16)
    equivalent = jnp.dot(state, pick, preferred_element_type=F32)
    center = jnp.sum(equivalent, axis=0, keepdims=True) * (1.0 / members)
    scaled = ((equivalent - center) * (members - 1) ** (-0.5)).astype(BF16)
    tail_row = lax.broadcasted_iota(jnp.int32, (16, nobs), 0)
    tail = jnp.where(
        tail_row == 0, val_v[...] - center, jnp.where(tail_row == 1, prec_v[...], 0.0)
    ).astype(BF16)
    for side in range(2):
        part = slice(side * half, (side + 1) * half)
        obs_own[side, 0:members] = scaled[:, part]
        obs_own[side, members : members + 16] = tail[:, part]
    swaps = [
        remote(obs_own.at[0], obs_in.at[1], obs_send.at[0], obs_recv.at[1], {"domain": west}),
        remote(obs_own.at[1], obs_in.at[0], obs_send.at[1], obs_recv.at[0], {"domain": east}),
    ]
    for copy in swaps:
        copy.start()

    ens_mean = jnp.sum(wide, axis=0, keepdims=True) * (1.0 / members)
    anomalies = (wide - ens_mean).astype(BF16)

    def term(block, which):
        rows = block[0:members]
        ends = block[members : members + 16]
        use = TAPER[which] * mask_v[0:1, which : which + 1].astype(F32)
        weight = ends[1:2].astype(F32) * use
        weighted = (rows.astype(F32) * weight).astype(BF16)
        part = lax.dot_general(rows, weighted, (((1,), (1,)), ((), ())), preferred_element_type=F32)
        push = lax.dot_general(weighted, ends, (((1,), (1,)), ((), ())), preferred_element_type=F32)
        return part, push[:, 0:1]

    cross, forcing = term(obs_own[0], 1)
    more, push = term(obs_own[1], 2)
    cross, forcing = cross + more, forcing + push
    swaps[1].wait_recv()
    more, push = term(obs_in[0], 0)
    cross, forcing = cross + more, forcing + push
    swaps[0].wait_recv()
    more, push = term(obs_in[1], 3)
    cross, forcing = cross + more, forcing + push

    cross_half = cross.astype(BF16)
    squared = jnp.dot(cross_half, cross_half, preferred_element_type=F32)
    sums = jnp.sum(jnp.abs(squared), axis=0, keepdims=True)
    bound = jnp.sqrt(jnp.max(sums, axis=1, keepdims=True))
    delta = (bound + 1.0) / 2.0
    theta = 1.0 + delta
    sigma = theta / delta
    rho0 = 1.0 / sigma
    rho1 = 1.0 / (2.0 * sigma - rho0)
    rest = 1.0 - 1.0 / theta
    keep = 1.0 + rho1 * rho0
    on_eye = 1.0 / theta + keep * rest / theta + 2.0 * rho1 / delta * rest * rest
    on_cross = -(keep + 4.0 * rho1) / (theta * theta)
    on_square = 2.0 * rho1 / (delta * theta * theta)
    eye = lax.broadcasted_iota(jnp.int32, (members, members), 0) == lax.broadcasted_iota(
        jnp.int32, (members, members), 1
    )
    inverse = jnp.where(eye, on_eye, 0.0) + on_cross * cross + on_square * squared
    mean_weights = jnp.sum(inverse * forcing, axis=0, keepdims=True)
    transform = (
        0.5 * (jnp.where(eye, 1.0, 0.0) + inverse) + mean_weights * (members - 1) ** (-0.5)
    ).astype(BF16)
    analysis = (
        ens_mean + jnp.dot(transform, anomalies, preferred_element_type=F32)
    ).astype(BF16)
    for i in range(count):
        back[i] = analysis[:, i * ncols : (i + 1) * ncols]
    returns = []
    for i in range(1, nm):
        copy = remote(
            back.at[:, mine(peers[i]), :], got.at[me_m], back_send.at[i], back_recv.at[i], {"member": peers[i]}
        )
        copy.start()
        returns.append(copy)
    got[me_m] = back[:, mine(me_m), :]
    for i in range(1, nm):
        remote(
            back.at[:, mine(froms[i]), :], got.at[froms[i]], back_send.at[i], back_recv.at[i], {"member": froms[i]}
        ).wait_recv()
    for copy in halos + sends + swaps + returns:
        copy.wait_send()


def solution(mesh):
    nm, nd = mesh.shape["member"], mesh.shape["domain"]

    def on_device(ensemble, obs_value, obs_prec, obs_row, obs_col, loc_mask):
        own, fields, nrows, ncols = ensemble.shape
        reg = nrows // nm
        members = own * nm
        nobs = obs_value.shape[1]
        layers = pl.cdiv(2 * fields * nrows, ncols)
        grant = 8 * 1024 * 1024 + 32 * members * members
        vm = pltpu.VMEM
        dma = pltpu.SemaphoreType.DMA
        parts = pl.pallas_call(
            functools.partial(kernel, nm, nd),
            out_shape=jax.ShapeDtypeStruct((nm, fields * reg, own, ncols), BF16),
            in_specs=[pl.BlockSpec(memory_space=pl.ANY)] * 6,
            out_specs=pl.BlockSpec(memory_space=pltpu.VMEM),
            scratch_shapes=[
                vm(ensemble.shape, BF16),
                vm((1, nobs), F32),
                vm((1, nobs), F32),
                vm((1, nobs), jnp.int32),
                vm((1, nobs), jnp.int32),
                vm(loc_mask.shape, jnp.int32),
                vm((own * fields * nrows, ncols), F32),
                vm((2, own, ncols), BF16),
                vm((2, own, ncols), BF16),
                vm((nm, fields * reg, own, ncols), BF16),
                vm((fields * reg, members, ncols), BF16),
                vm((layers, own, ncols), BF16),
                vm((layers, members, ncols), BF16),
                vm((2, members + 16, nobs // 2), BF16),
                vm((2, members + 16, nobs // 2), BF16),
                vm((fields * reg, members, ncols), BF16),
                dma((6,)),
                dma((2,)),
                dma((2,)),
                dma((nm,)),
                dma((nm,)),
                dma((nm,)),
                dma((nm,)),
                dma((2,)),
                dma((2,)),
                dma((nm,)),
                dma((nm,)),
            ],
            compiler_params=pltpu.CompilerParams(collective_id=0, has_side_effects=True, vmem_limit_bytes=grant),
        )(*(pltpu.with_memory_space_constraint(x, pltpu.HBM) for x in (ensemble, obs_value, obs_prec, obs_row, obs_col, loc_mask)))
        parts = parts.reshape(nm, fields, reg, own, ncols)
        return jnp.transpose(parts, (3, 1, 0, 2, 4)).reshape(ensemble.shape)

    in_specs = (P("member", None, None, "domain"),) + (P("member", "domain"),) * 5
    return jax.shard_map(
        on_device, mesh=mesh, in_specs=in_specs, out_specs=P("member", None, None, "domain"), check_vma=False
    )
```

```python
import functools

import jax
import jax.numpy as jnp
from jax import lax
from jax.experimental import pallas as pl
from jax.experimental.pallas import tpu as pltpu
from jax.sharding import PartitionSpec as P

ADVECT = 0.4
DIFFUSE = 0.15
OBS_WIND = 0.5
TAPER = (0.5, 1.0, 1.0, 0.5)
MESH = pl.DeviceIdType.MESH
F32 = jnp.float32
BF16 = jnp.bfloat16


def remote(src, dst, send, recv, where):
    return pltpu.make_async_remote_copy(
        src_ref=src, dst_ref=dst, send_sem=send, recv_sem=recv, device_id=where, device_id_type=MESH
    )


def kernel(
    nm, nd, ens, value, prec, row, col, mask, got,
    raw, val_v, prec_v, row_v, col_v, mask_v, rows_f32, halo_out, halo_in, bands, cells, edge_out, edge_in, obs_own, obs_in,
    back, load_sem, halo_send, halo_recv, out_send, out_recv, edge_send, edge_recv, obs_send, obs_recv, back_send, back_recv,
):
    me_m = lax.axis_index("member")
    me_d = lax.axis_index("domain")
    east = lax.rem(me_d + 1, nd)
    west = lax.rem(me_d + nd - 1, nd)
    peers = [lax.rem(me_m + i, nm) for i in range(nm)]
    froms = [lax.rem(me_m + nm - i, nm) for i in range(nm)]
    own, fields, nrows, ncols = raw.shape
    reg = nrows // nm
    members = own * nm
    pitch = fields * nrows

    barrier = pltpu.get_barrier_semaphore()
    for i in range(1, nm):
        pl.semaphore_signal(barrier, inc=1, device_id={"member": peers[i]}, device_id_type=MESH)
    for near in (east, west):
        pl.semaphore_signal(barrier, inc=1, device_id={"domain": near}, device_id_type=MESH)
    loads = [
        pltpu.make_async_copy(src, dst, load_sem.at[i])
        for i, (src, dst) in enumerate(
            [(ens, raw), (value, val_v), (prec, prec_v), (row, row_v), (col, col_v), (mask, mask_v)]
        )
    ]
    for load in loads:
        load.start()
    loads[0].wait()

    rows_f32[...] = raw[...].astype(F32).reshape(own * pitch, ncols)

    def line(f, r):
        return rows_f32[pl.ds(f * nrows + (r % nrows if isinstance(r, int) else lax.rem(r, nrows)), own, stride=pitch), :]

    lane = lax.broadcasted_iota(jnp.int32, (own, ncols), 1)
    used = fields * nrows

    def packed(column):
        total = jnp.zeros((own, ncols), F32)
        for f in range(fields):
            for r in range(nrows):
                spot = f * nrows + r
                moved = pltpu.roll(line(f, r), (spot - column) % ncols, 1)
                total = jnp.where(lane == spot, moved, total)
        return total

    first, last = packed(0), packed(ncols - 1)
    halo_out[0] = first.astype(BF16)
    halo_out[1] = last.astype(BF16)
    pl.semaphore_wait(barrier, nm + 1)
    halos = [
        remote(halo_out.at[0], halo_in.at[0], halo_send.at[0], halo_recv.at[0], {"domain": west}),
        remote(halo_out.at[1], halo_in.at[1], halo_send.at[1], halo_recv.at[1], {"domain": east}),
    ]
    for copy in halos:
        copy.start()

    def mine(block):
        return pl.ds(pl.multiple_of(block * own, own), own)

    def step(middle, east_side, west_side, north, south, wind):
        laplace = east_side + west_side + north + south - 4.0 * middle
        return (middle - ADVECT * 0.5 * wind * (east_side - west_side) + DIFFUSE * laplace).astype(BF16)

    def interior(m, f, r):
        at = m * reg + r
        middle = line(f, at)
        return step(
            middle, pltpu.roll(middle, ncols - 1, 1), pltpu.roll(middle, 1, 1),
            line(f, at + 1), line(f, at + nrows - 1), line(0, at),
        )

    sends = []
    for i in list(range(1, nm)) + [0]:
        m = peers[i]
        for f in range(fields):
            for r in range(reg):
                if i:
                    bands[i, f * reg + r] = interior(m, f, r)
                else:
                    cells[f * reg + r, mine(me_m), :] = interior(m, f, r)
        if i:
            copy = remote(bands.at[i], cells.at[:, mine(me_m), :], out_send.at[i], out_recv.at[i], {"member": m})
            copy.start()
            sends.append(copy)

    second, prior = packed(1), packed(ncols - 2)
    row_of = lax.rem(lane, nrows)

    def north_of(x):
        return jnp.where(row_of == nrows - 1, pltpu.roll(x, nrows - 1, 1), pltpu.roll(x, ncols - 1, 1))

    def south_of(x):
        return jnp.where(row_of == 0, pltpu.roll(x, ncols - nrows + 1, 1), pltpu.roll(x, 1, 1))

    def wind_of(x):
        total = x
        for f in range(1, fields):
            total = jnp.where(lane // nrows == f, pltpu.roll(x, f * nrows, 1), total)
        return total

    for copy in halos:
        copy.wait_recv()
    edge_first = step(
        first, second, halo_in[1].astype(F32), north_of(first), south_of(first), wind_of(first)
    )
    edge_last = step(
        last, halo_in[0].astype(F32), prior, north_of(last), south_of(last), wind_of(last)
    )
    layers = edge_out.shape[0]
    if layers == 1:
        edge_out[0] = jnp.where(
            lane < used, edge_first.astype(F32), pltpu.roll(edge_last.astype(F32), used, 1)
        ).astype(BF16)
    else:
        edge_out[0] = edge_first
        edge_out[1] = edge_last
    for i in range(1, nm):
        copy = remote(
            edge_out, edge_in.at[:, mine(me_m), :], edge_send.at[i], edge_recv.at[i], {"member": peers[i]}
        )
        copy.start()
        sends.append(copy)
    for k in range(layers):
        edge_in[k, mine(me_m), :] = edge_out[k]

    for load in loads[1:]:
        load.wait()
    nobs = val_v.shape[1]
    half = nobs // 2
    index = row_v[...] * ncols + col_v[...]
    spots = lax.broadcasted_iota(jnp.int32, (reg * ncols, nobs), 0)
    hit = jnp.where(spots == index, 1.0, 0.0)
    pick = jnp.concatenate([(OBS_WIND * hit).astype(BF16), hit.astype(BF16)], axis=0)

    for i in range(1, nm):
        remote(
            bands.at[i], cells.at[:, mine(froms[i]), :], out_send.at[i], out_recv.at[i], {"member": froms[i]}
        ).wait_recv()
    for i in range(1, nm):
        remote(
            edge_out, edge_in.at[:, mine(froms[i]), :], edge_send.at[i], edge_recv.at[i], {"member": froms[i]}
        ).wait_recv()
    lead = lax.rem(ncols - me_m * reg, ncols)
    edges = [pltpu.roll(edge_in[k].astype(F32), lead, 1) for k in range(layers)]
    wide_lane = lax.broadcasted_iota(jnp.int32, (members, ncols), 1)

    def whole(f, r):
        spot = f * nrows + r
        left = edges[0][:, spot : spot + 1]
        if layers == 1:
            right = edges[0][:, used + spot : used + spot + 1]
        else:
            right = edges[1][:, spot : spot + 1]
        shape = (members, ncols)
        inner = cells[f * reg + r].astype(F32)
        inner = jnp.where(wide_lane == 0, jnp.broadcast_to(left, shape), inner)
        return jnp.where(wide_lane == ncols - 1, jnp.broadcast_to(right, shape), inner)

    count = fields * reg
    wide = jnp.concatenate([whole(f, r) for f in range(fields) for r in range(reg)], axis=1)
    state = wide.astype(BF16)
    equivalent = jnp.dot(state, pick, preferred_element_type=F32)
    center = jnp.sum(equivalent, axis=0, keepdims=True) * (1.0 / members)
    scaled = ((equivalent - center) * (members - 1) ** (-0.5)).astype(BF16)
    tail_row = lax.broadcasted_iota(jnp.int32, (16, nobs), 0)
    tail = jnp.where(
        tail_row == 0, val_v[...] - center, jnp.where(tail_row == 1, prec_v[...], 0.0)
    ).astype(BF16)
    for side in range(2):
        part = slice(side * half, (side + 1) * half)
        obs_own[side, 0:members] = scaled[:, part]
        obs_own[side, members : members + 16] = tail[:, part]
    swaps = [
        remote(obs_own.at[0], obs_in.at[1], obs_send.at[0], obs_recv.at[1], {"domain": west}),
        remote(obs_own.at[1], obs_in.at[0], obs_send.at[1], obs_recv.at[0], {"domain": east}),
    ]
    for copy in swaps:
        copy.start()

    ens_mean = jnp.sum(wide, axis=0, keepdims=True) * (1.0 / members)
    anomalies = (wide - ens_mean).astype(BF16)

    def term(blocks, whichs):
        block = jnp.concatenate(blocks, axis=1)
        rows = block[0:members]
        ends = block[members : members + 16]
        use = jnp.concatenate(
            [
                jnp.broadcast_to(TAPER[which] * mask_v[0:1, which : which + 1].astype(F32), (1, half))
                for which in whichs
            ],
            axis=1,
        )
        weight = ends[1:2].astype(F32) * use
        weighted = (rows.astype(F32) * weight).astype(BF16)
        part = lax.dot_general(rows, weighted, (((1,), (1,)), ((), ())), preferred_element_type=F32)
        push = lax.dot_general(weighted, ends, (((1,), (1,)), ((), ())), preferred_element_type=F32)
        return part, push[:, 0:1]

    cross, forcing = term([obs_own[0], obs_own[1]], (1, 2))
    swaps[1].wait_recv()
    swaps[0].wait_recv()
    more, push = term([obs_in[0], obs_in[1]], (0, 3))
    cross, forcing = cross + more, forcing + push

    cross_half = cross.astype(BF16)
    squared = jnp.dot(cross_half, cross_half, preferred_element_type=F32)
    sums = jnp.sum(jnp.abs(squared), axis=0, keepdims=True)
    bound = jnp.sqrt(jnp.max(sums, axis=1, keepdims=True))
    delta = (bound + 1.0) / 2.0
    theta = 1.0 + delta
    sigma = theta / delta
    rho0 = 1.0 / sigma
    rho1 = 1.0 / (2.0 * sigma - rho0)
    rest = 1.0 - 1.0 / theta
    keep = 1.0 + rho1 * rho0
    on_eye = 1.0 / theta + keep * rest / theta + 2.0 * rho1 / delta * rest * rest
    on_cross = -(keep + 4.0 * rho1) / (theta * theta)
    on_square = 2.0 * rho1 / (delta * theta * theta)
    eye = lax.broadcasted_iota(jnp.int32, (members, members), 0) == lax.broadcasted_iota(
        jnp.int32, (members, members), 1
    )
    inverse = jnp.where(eye, on_eye, 0.0) + on_cross * cross + on_square * squared
    mean_weights = jnp.sum(inverse * forcing, axis=0, keepdims=True)
    transform = (
        0.5 * (jnp.where(eye, 1.0, 0.0) + inverse) + mean_weights * (members - 1) ** (-0.5)
    ).astype(BF16)
    analysis = (
        ens_mean + jnp.dot(transform, anomalies, preferred_element_type=F32)
    ).astype(BF16)
    for i in range(count):
        back[i] = analysis[:, i * ncols : (i + 1) * ncols]
    returns = []
    for i in range(1, nm):
        copy = remote(
            back.at[:, mine(peers[i]), :], got.at[me_m], back_send.at[i], back_recv.at[i], {"member": peers[i]}
        )
        copy.start()
        returns.append(copy)
    got[me_m] = back[:, mine(me_m), :]
    for i in range(1, nm):
        remote(
            back.at[:, mine(froms[i]), :], got.at[froms[i]], back_send.at[i], back_recv.at[i], {"member": froms[i]}
        ).wait_recv()
    for copy in halos + sends + swaps + returns:
        copy.wait_send()


def solution(mesh):
    nm, nd = mesh.shape["member"], mesh.shape["domain"]

    def on_device(ensemble, obs_value, obs_prec, obs_row, obs_col, loc_mask):
        own, fields, nrows, ncols = ensemble.shape
        reg = nrows // nm
        members = own * nm
        nobs = obs_value.shape[1]
        layers = pl.cdiv(2 * fields * nrows, ncols)
        grant = 8 * 1024 * 1024 + 32 * members * members
        vm = pltpu.VMEM
        dma = pltpu.SemaphoreType.DMA
        parts = pl.pallas_call(
            functools.partial(kernel, nm, nd),
            out_shape=jax.ShapeDtypeStruct((nm, fields * reg, own, ncols), BF16),
            in_specs=[pl.BlockSpec(memory_space=pl.ANY)] * 6,
            out_specs=pl.BlockSpec(memory_space=pltpu.VMEM),
            scratch_shapes=[
                vm(ensemble.shape, BF16),
                vm((1, nobs), F32),
                vm((1, nobs), F32),
                vm((1, nobs), jnp.int32),
                vm((1, nobs), jnp.int32),
                vm(loc_mask.shape, jnp.int32),
                vm((own * fields * nrows, ncols), F32),
                vm((2, own, ncols), BF16),
                vm((2, own, ncols), BF16),
                vm((nm, fields * reg, own, ncols), BF16),
                vm((fields * reg, members, ncols), BF16),
                vm((layers, own, ncols), BF16),
                vm((layers, members, ncols), BF16),
                vm((2, members + 16, nobs // 2), BF16),
                vm((2, members + 16, nobs // 2), BF16),
                vm((fields * reg, members, ncols), BF16),
                dma((6,)),
                dma((2,)),
                dma((2,)),
                dma((nm,)),
                dma((nm,)),
                dma((nm,)),
                dma((nm,)),
                dma((2,)),
                dma((2,)),
                dma((nm,)),
                dma((nm,)),
            ],
            compiler_params=pltpu.CompilerParams(collective_id=0, has_side_effects=True, vmem_limit_bytes=grant),
        )(*(pltpu.with_memory_space_constraint(x, pltpu.HBM) for x in (ensemble, obs_value, obs_prec, obs_row, obs_col, loc_mask)))
        parts = parts.reshape(nm, fields, reg, own, ncols)
        return jnp.transpose(parts, (3, 1, 0, 2, 4)).reshape(ensemble.shape)

    in_specs = (P("member", None, None, "domain"),) + (P("member", "domain"),) * 5
    return jax.shard_map(
        on_device, mesh=mesh, in_specs=in_specs, out_specs=P("member", None, None, "domain"), check_vma=False
    )
```
